32 devices in a mesh: patch: 8 (over z, y), dir: 4 (over x, core).
Axes of the slice: x: 2, y: 2, z: 4, core: 2. Of those that a mesh axis runs over, the one named last changes fastest.
Arguments:
- right_side: float32 [96, 192, 256], P('dir', 'patch'), may hold values from -6 to 6
- guess: float32 [96, 192, 256], P('dir', 'patch'), may hold values from -3 to 3
- mask_fine: int32 [96, 192, 2], P('dir', 'patch'), may hold values 0 or 1
- mask_next: int32 [48, 96, 1], P('dir', 'patch'), may hold values 0 or 1
Outputs:
- solution: float32 [96, 192, 256], P('dir', 'patch')
The draws below stay inside these ranges and needn't reach their ends.
All inputs are finite; a program needn't handle non-finite values. No bound on the sum of `mask_fine` or of `mask_next` on one device may be relied on, other than what follows from the above.
Results may differ from the reference program's by a relative error of at most 0.00005.
Values sent between devices are 32-bit elements; how exact they have to be, the bound alone decides.
A program may use at most 64 MiB of HBM per device.

```python
import jax
import jax.numpy as jnp
from jax import lax

NW = 256
TILE = 128
SWEEPS = 3
LEVELS = 4
NU = 96
NV = 192


def with_ends(result, rng, low, top_value):
    index_at = [jax.random.randint(jax.random.fold_in(rng, axis), (), 0, length) for axis, length in enumerate(result.shape)]
    main_axis = result.shape.index(max(result.shape))
    neighbour = index_at[:main_axis] + [(index_at[main_axis] + 1) % result.shape[main_axis]] + index_at[main_axis + 1:]
    return result.at[tuple(index_at)].set(low).at[tuple(neighbour)].set(top_value)


def steps_of(rng, extent, cuts, smallest, largest):
    level, own = 1.0, jax.random.fold_in(rng, 6)
    for dim, blocks in cuts:
        steps = jnp.exp(jax.random.uniform(jax.random.fold_in(own, dim), (blocks,), jnp.float32, smallest / len(cuts), largest / len(cuts)))
        level = level * jnp.repeat(steps, extent[dim] // blocks).reshape([-1 if axis == dim else 1 for axis in range(len(extent))])
    return level


def normal_values(rng, dims, scale, most, shards=(), kind=jnp.bfloat16):
    values = jax.random.normal(rng, dims, jnp.float32) * scale
    if len(shards) > 0:
        values = steps_of(rng, dims, shards, -0.22, 0.18) * values
    return jnp.clip(values, min=-most, max=most).astype(kind)


def setup_inputs(seed: int = 0) -> dict:
    arg_keys = jax.random.split(jax.random.key(seed), 5)
    right_side = normal_values(arg_keys[0], (NU, NV, NW), 1.0, 6.0, ((0, 4), (1, 8)), jnp.float32)
    guess = normal_values(arg_keys[1], (NU, NV, NW), 0.5, 3.0, ((0, 4), (1, 8)), jnp.float32)
    mask_fine = with_ends((jax.random.randint(arg_keys[2], (NU, NV, NW // TILE), 0, 4) < 3).astype(jnp.int32), jax.random.fold_in(arg_keys[2], 1), 0, 1)
    mask_next = with_ends((jax.random.randint(arg_keys[3], (NU // 2, NV // 2, NW // (2 * TILE)), 0, 4) < 3).astype(jnp.int32), jax.random.fold_in(arg_keys[3], 1), 0, 1)
    return {"right_side": right_side, "guess": guess, "mask_fine": mask_fine, "mask_next": mask_next}


MASS = (1.0 / 5040, 120.0 / 5040, 1191.0 / 5040, 2416.0 / 5040, 1191.0 / 5040, 120.0 / 5040, 1.0 / 5040)
STIFF = (-1.0 / 120, -0.2, -0.125, 2.0 / 3, -0.125, -0.2, -1.0 / 120)
SUBDIV = (0.125, 0.5, 0.75, 0.5, 0.125)
OMEGA = 0.5


def wrap_pad(values, dimension, width, periodic):
    length = values.shape[dimension]
    if periodic:
        return jnp.concatenate([lax.slice_in_dim(values, length - width, length, axis=dimension), values, lax.slice_in_dim(values, 0, width, axis=dimension)], axis=dimension)
    widths = [(0, 0)] * values.ndim
    widths[dimension] = (width, width)
    return jnp.pad(values, widths)


def band_line(values, dimension, stencil, periodic):
    length = values.shape[dimension]
    padded = wrap_pad(values, dimension, 3, periodic)
    running = stencil[0] * lax.slice_in_dim(padded, 0, length, axis=dimension)
    for offset in range(1, 7):
        running = running + stencil[offset] * lax.slice_in_dim(padded, offset, offset + length, axis=dimension)
    return running


def restrict_line(values, dimension, periodic):
    halved = values.shape[dimension] // 2
    padded = wrap_pad(values, dimension, 2, periodic)
    running = SUBDIV[0] * lax.slice_in_dim(padded, 0, 2 * halved - 1, stride=2, axis=dimension)
    for offset in range(1, 5):
        running = running + SUBDIV[offset] * lax.slice_in_dim(padded, offset, offset + 2 * halved - 1, stride=2, axis=dimension)
    return running


def prolong_line(values, dimension, periodic):
    length = values.shape[dimension]
    padded = wrap_pad(values, dimension, 1, periodic)
    upper_part = lax.slice_in_dim(padded, 2, length + 2, axis=dimension)
    middle_part = lax.slice_in_dim(padded, 1, length + 1, axis=dimension)
    lower_part = lax.slice_in_dim(padded, 0, length, axis=dimension)
    even_part = SUBDIV[0] * upper_part + SUBDIV[2] * middle_part + SUBDIV[4] * lower_part
    odd_part = SUBDIV[1] * upper_part + SUBDIV[3] * middle_part
    joined = jnp.stack([even_part, odd_part], axis=dimension + 1)
    old_shape = values.shape
    return joined.reshape(old_shape[:dimension] + (2 * length,) + old_shape[dimension + 1:])


def operate(current, scale_factor):
    mass_side = band_line(current, 2, MASS, False)
    stiff_side = band_line(current, 2, STIFF, False)
    first_term = band_line(mass_side, 1, MASS, True)
    second = band_line(mass_side, 1, STIFF, True) + band_line(stiff_side, 1, MASS, True)
    return scale_factor * (band_line(first_term, 0, STIFF, False) + band_line(second, 0, MASS, False))


def smooth(current, load, scale_factor, active):
    update = (OMEGA / scale_factor) * (load - operate(current, scale_factor))
    if active is not None:
        update = update * active
    return current + update


def cycle(load, current, level_index, actives):
    scale_factor = float(2 ** level_index)
    active = actives[level_index]
    for sweep_index in range(SWEEPS):
        current = smooth(current, load, scale_factor, active)
    if level_index + 1 < LEVELS:
        residual_field = load - operate(current, scale_factor)
        if active is not None:
            residual_field = residual_field * active
        coarse_load = restrict_line(restrict_line(restrict_line(residual_field, 2, False), 1, True), 0, False)
        correction = cycle(coarse_load, jnp.zeros_like(coarse_load), level_index + 1, actives)
        finer = prolong_line(prolong_line(prolong_line(correction, 2, False), 1, True), 0, False)
        if active is not None:
            finer = finer * active
        current = current + finer
    for sweep_index in range(SWEEPS):
        current = smooth(current, load, scale_factor, active)
    return current


def reference(right_side, guess, mask_fine, mask_next):
    actives = [jnp.repeat(mask_fine.astype(jnp.float32), TILE, axis=2), jnp.repeat(mask_next.astype(jnp.float32), TILE, axis=2)] + [None] * (LEVELS - 2)
    return cycle(right_side, guess * actives[0], 0, actives)
```

```python
import functools

import jax
import jax.numpy as jnp
import numpy as np
from jax import lax
from jax.experimental import pallas as pl
from jax.experimental.pallas import tpu as pltpu
from jax.sharding import PartitionSpec as P

TILE = 128
SWEEPS = 3
LEVELS = 4
MASS = tuple(v / 5040 for v in (1, 120, 1191, 2416, 1191, 120, 1))
STIFF = tuple(v / 120 for v in (-1, -24, -15, 80, -15, -24, -1))
SUBDIV = (0.125, 0.5, 0.75, 0.5, 0.125)
OMEGA = 0.5
MESH = pl.DeviceIdType.MESH
WAYS = ((0, 1), (0, -1), (1, 0), (1, 1), (1, -1), (-1, 0), (-1, 1), (-1, -1))


def up8(n):
    return -(-n // 8) * 8


def band(n, size, coeffs):
    i, j = np.indices((size, size))
    out = np.zeros((size, size), np.float32)
    for k, c in enumerate(coeffs):
        out[(j - i + 3 == k) & (i < n) & (j < n)] = c
    return out


def subdivision(n, rows, columns):
    i, j = np.indices((rows, columns))
    out = np.zeros((rows, columns), np.float32)
    for k, c in enumerate(SUBDIV):
        out[(i - 2 * j + 2 == k) & (i < 2 * n) & (j < n)] = c
    return out


def weights(width):
    bands, moves = [], []
    for level in range(LEVELS):
        n = width >> level
        size = max(n, 128)
        mass = band(n, size, (1, 120, 1191, 2416, 1191, 120, 1))
        high = mass.astype(jnp.bfloat16)
        low = (mass - high.astype(np.float32)).astype(jnp.bfloat16)
        stiff = band(n, size, (-1, -24, -15, 80, -15, -24, -1)).astype(jnp.bfloat16)
        bands.append(np.stack([high, low, stiff]))
        if level + 1 < LEVELS:
            move = subdivision(n // 2, size, max(n // 2, 128))
            moves.append((move.astype(jnp.bfloat16), np.ascontiguousarray(move.T).astype(jnp.bfloat16)))
    return bands, moves


def parts(x):
    high = x.astype(jnp.bfloat16)
    return high, (x - high.astype(jnp.float32)).astype(jnp.bfloat16)


def mul(a, b):
    return jnp.dot(a, b, preferred_element_type=jnp.float32)


def taps(x, coeffs):
    sums = (x[0] + x[6], x[1] + x[5], x[2] + x[4], x[3])
    total = coeffs[3] * sums[3]
    for k in range(3):
        total = total + coeffs[k] * sums[k]
    return total


def kernel(sets, n_dir, n_patch, rs, guess, s0, s1, *refs):
    bands, refs = refs[:LEVELS], refs[LEVELS:]
    moves, refs = refs[: 2 * (LEVELS - 1)], refs[2 * (LEVELS - 1) :]
    out, refs = refs[0], refs[1:]
    bufs = []
    for _ in sets:
        bufs.append(refs[:6])
        refs = refs[6:]
    fields = []
    for level in range(LEVELS):
        fields.append(refs[:6])
        refs = refs[6:]
    send_sem, recv_sem = refs
    masks = (s0, s1, None, None)

    me_u, me_v = lax.axis_index("dir"), lax.axis_index("patch")
    has_down, has_up = me_u > 0, me_u < n_dir - 1

    def device(a, b):
        return {"dir": me_u + a, "patch": lax.rem(me_v + b + n_patch, n_patch)}

    def when_way(a, body):
        if a == 0:
            body()
        else:
            pl.when(has_up if a > 0 else has_down)(body)

    barrier = pltpu.get_barrier_semaphore()
    for step in (0, 1, -1):
        def greet():
            for a, b in WAYS:
                if a == step:
                    pl.semaphore_signal(barrier, inc=1, device_id=device(a, b), device_id_type=MESH)
        when_way(step, greet)

    for (nu, nv, nvp, w), (c, sl, sr, rl, rr, p) in zip(sets, bufs):
        p[:, nvp + 8 :, :] = jnp.zeros((nu + 6, 8, w), jnp.float32)
        for flag, at in ((me_u == 0, 0), (me_u == n_dir - 1, nu + 3)):
            @pl.when(flag)
            def _():
                c[:, at : at + 3] = jnp.zeros((2, 3, nvp, w), jnp.float32)
                rl[:, at : at + 3] = jnp.zeros((2, 3, 3, w), jnp.float32)
                rr[:, at : at + 3] = jnp.zeros((2, 3, 3, w), jnp.float32)

    inside = jnp.logical_and(has_down, has_up)
    pl.when(inside)(lambda: pl.semaphore_wait(barrier, 8))
    pl.when(jnp.logical_not(inside))(lambda: pl.semaphore_wait(barrier, 5))

    def exchange(which, x, number):
        nu, nv, nvp, w = sets[which]
        c, sl, sr, rl, rr, p = bufs[which]
        slot = lax.rem(number, 2)

        def stage(u, _):
            row = x[u]
            c[slot, u + 3] = row
            sl[slot, u] = row[0:3]
            sr[slot, u] = row[nv - 3 : nv]
            return 0

        lax.fori_loop(0, nu, stage, 0, unroll=min(nu, 4))

        def copy(index):
            a, b = WAYS[index]
            if b == 0:
                at, to = (nu, 0) if a > 0 else (3, nu + 3)
                src, dst = c.at[slot, at : at + 3], c.at[slot, to : to + 3]
            else:
                near, far = (sr, rl) if b > 0 else (sl, rr)
                if a == 0:
                    src, dst = near.at[slot], far.at[slot, 3 : nu + 3]
                else:
                    at, to = (nu - 3, 0) if a > 0 else (0, nu + 3)
                    src, dst = near.at[slot, at : at + 3], far.at[slot, to : to + 3]
            return pltpu.make_async_remote_copy(
                src_ref=src,
                dst_ref=dst,
                send_sem=send_sem.at[slot, index],
                recv_sem=recv_sem.at[slot, index],
                device_id=device(a, b),
                device_id_type=MESH,
            )

        for step in (1, -1, 0):
            def start():
                for index, (a, b) in enumerate(WAYS):
                    if a == step:
                        copy(index).start()
            when_way(step, start)
        for step in (0, 1, -1):
            def finish():
                for index, (a, b) in enumerate(WAYS):
                    if a == step:
                        copy(index).wait_send()
                    if a == -step:
                        copy(index).wait_recv()
            when_way(step, finish)

        def gather(u, _):
            p[u, 8 : 8 + nvp] = c[slot, u]
            p[u, 5:8] = rl[slot, u]
            p[u, 8 + nv : 11 + nv] = rr[slot, u]
            return 0

        lax.fori_loop(0, nu + 6, gather, 0, unroll=3)

    def chunked(which, body):
        nu, nv, nvp, w = sets[which]
        size = nu
        while size * nvp > 192 and size % 2 == 0:
            size //= 2
        if size == nu:
            body(0, nu)
        else:
            lax.fori_loop(0, nu // size, lambda i, _: (body(i * size, size), 0)[1], 0)

    def operate(level, x, number, use):
        which = set_of[level]
        nu, nv, nvp, w = sets[which]
        p = bufs[which][5]
        load, field, pu, ku, g, h = fields[level]
        exchange(which, x, number)

        def sublanes(u, _):
            t = [p[u, 5 + k : 5 + k + nvp, :] for k in range(7)]
            pu[u] = taps(t, [v / 5040 for v in MASS])
            ku[u] = taps(t, [v / 5040 for v in STIFF])
            return 0

        lax.fori_loop(0, nu + 6, sublanes, 0, unroll=2)

        def leading(u, _):
            a = [pu[u + k] for k in range(7)]
            b = [ku[u + k] for k in range(7)]
            g[u] = taps(a, STIFF) + taps(b, MASS)
            h[u] = taps(a, [v * 42 for v in MASS])
            return 0

        lax.fori_loop(0, nu, leading, 0, unroll=2)
        table = bands[level]

        def finish(u, size):
            g_high, g_low = parts(g[pl.ds(u, size)].reshape(size * nvp, w))
            h_high, h_low = parts(h[pl.ds(u, size)].reshape(size * nvp, w))
            value = mul(g_high, table[0]) + mul(g_low, table[0]) + mul(g_high, table[1])
            value = value + mul(h_high, table[2]) + mul(h_low, table[2])
            use(pl.ds(u, size), value.reshape(size, nvp, w))

        chunked(which, finish)

    def sweep(level, number):
        load, field = fields[level][:2]
        mask = masks[level]

        def use(at, value):
            update = (OMEGA / 2**level) * load[at] - OMEGA * value
            if mask is not None:
                update = update * mask[at]
            field[at] = field[at] + update

        operate(level, field, number, use)

    def sweeps(level, count, number):
        def body(i, _):
            sweep(level, number + i)
            return 0

        lax.fori_loop(0, count, body, 0)
        return number + count

    def descend(level, number):
        which = set_of[level]
        nu, nv, nvp, w = sets[which]
        load, field, pu, ku, g, h = fields[level]
        mask = masks[level]
        if level == 0:
            number = sweeps(level, SWEEPS, number)
        else:
            first = (OMEGA / 2**level) * load[...]
            field[...] = first if mask is None else first * mask[...]
            number = sweeps(level, SWEEPS - 1, number)
        if level + 1 < LEVELS:
            low_which = 1 if level == 0 else which
            low_p = bufs[low_which][5]
            down, up = moves[2 * level], moves[2 * level + 1]
            lanes = down.shape[1]

            def residual(at, value):
                r = load[at] - float(2**level) * value
                if mask is not None:
                    r = r * mask[at]
                size = r.shape[0]
                r_high, r_low = parts(r.reshape(size * nvp, w))
                n = mul(r_high, down[...]) + mul(r_low, down[...])
                g[at, :, 0:lanes] = n.reshape(size, nvp, lanes)

            operate(level, field, number, residual)
            number += 1
            exchange(low_which, g.at[:, :, 0:lanes], number)
            number += 1
            cu, cv, cvp, cw = sets[set_of[level + 1]]
            c_load, c_field = fields[level + 1][:2]
            c_p = bufs[set_of[level + 1]][5]
            c_load[...] = jnp.zeros((cu, cvp, cw), jnp.float32)
            for i in range(cu):
                total = None
                for k in range(5):
                    line = None
                    for m in range(5):
                        term = SUBDIV[m] * low_p[2 * i + k + 1, pl.ds(6 + m, cv, stride=2), :]
                        line = term if line is None else line + term
                    total = SUBDIV[k] * line if total is None else total + SUBDIV[k] * line
                c_load[i, 0:cv, :] = total
            number = descend(level + 1, number)
            exchange(set_of[level + 1], c_field, number)
            number += 1
            for u in range(nu):
                i = u // 2 + 3
                mix = ((i - 1, 0.125), (i, 0.75), (i + 1, 0.125)) if u % 2 == 0 else ((i, 0.5), (i + 1, 0.5))
                shifted = []
                for d in range(3):
                    total = None
                    for row, c in mix:
                        term = c * c_p[row, 7 + d : 7 + d + cv, :]
                        total = term if total is None else total + term
                    shifted.append(total)
                before, here, after = shifted
                spread[level][u, pl.ds(0, cv, stride=2), :] = 0.125 * (before + after) + 0.75 * here
                spread[level][u, pl.ds(1, cv, stride=2), :] = 0.5 * (here + after)

            def correct(at, size):
                at = pl.ds(at, size)
                y_high, y_low = parts(spread[level][at].reshape(size * nvp, lanes))
                y = (mul(y_high, up[...]) + mul(y_low, up[...])).reshape(size, nvp, w)
                if mask is not None:
                    y = y * mask[at]
                field[at] = field[at] + y

            chunked(which, correct)
        return sweeps(level, SWEEPS, number)

    set_of = [0, 2, 3, 4]
    spread = [bufs[1][0].at[0]] + [fields[level][3] for level in range(1, LEVELS)]
    load, field = fields[0][:2]
    load[...] = rs[...]
    field[...] = guess[...] * s0[...]
    descend(0, 0)
    out[...] = field[...]


def on_device(right_side, guess, mask_fine, mask_next):
    nu, nv, nw = right_side.shape
    sets = [(nu, nv, up8(nv), nw), (nu, nv, up8(nv), max(nw // 2, 128))]
    for level in range(1, LEVELS):
        sets.append((nu >> level, nv >> level, up8(nv >> level), max(nw >> level, 128)))
    sets = tuple(sets)
    bands, moves = weights(nw)
    s0 = jnp.repeat(mask_fine.astype(jnp.float32), TILE, axis=2)
    s1 = jnp.repeat(mask_next.astype(jnp.float32), TILE, axis=2)
    s1 = jnp.pad(s1, ((0, 0), (0, sets[2][2] - sets[2][1]), (0, sets[2][3] - s1.shape[2])))
    operands = [right_side, guess, s0, s1] + [jnp.asarray(b) for b in bands]
    operands += [jnp.asarray(m) for pair in moves for m in pair]
    scratch = []
    for u, v, vp, w in sets:
        scratch += [pltpu.VMEM((2, u + 6, vp, w), jnp.float32)]
        scratch += [pltpu.VMEM((2, u, 3, w), jnp.float32)] * 2
        scratch += [pltpu.VMEM((2, u + 6, 3, w), jnp.float32)] * 2
        scratch += [pltpu.VMEM((u + 6, vp + 16, w), jnp.float32)]
    for which in (0, 2, 3, 4):
        u, v, vp, w = sets[which]
        scratch += [pltpu.VMEM((u, vp, w), jnp.float32)] * 2
        scratch += [pltpu.VMEM((u + 6, vp, w), jnp.float32)] * 2
        scratch += [pltpu.VMEM((u, vp, w), jnp.float32)] * 2
    scratch += [pltpu.SemaphoreType.DMA((2, 8)), pltpu.SemaphoreType.DMA((2, 8))]
    vmem = pl.BlockSpec(memory_space=pltpu.VMEM)
    return pl.pallas_call(
        functools.partial(kernel, sets, lax.axis_size("dir"), lax.axis_size("patch")),
        out_shape=jax.ShapeDtypeStruct(right_side.shape, jnp.float32),
        in_specs=[vmem] * len(operands),
        out_specs=vmem,
        scratch_shapes=scratch,
        compiler_params=pltpu.CompilerParams(
            collective_id=0, has_side_effects=True, vmem_limit_bytes=60 * 2**20
        ),
        name="vcycle",
    )(*operands)


def solution(mesh):
    spec = P("dir", "patch", None)
    return jax.shard_map(
        on_device, mesh=mesh, in_specs=(spec,) * 4, out_specs=spec, check_vma=False
    )
```
